32 devices in a mesh: dp: 1 (over z), tp: 4 (over y), ep: 8 (over x, core).
Axes of the slice: x: 4, y: 4, z: 1, core: 2. Of those that a mesh axis runs over, the one named last changes fastest.
The devices are a block of a 4x4x8 slice.
Arguments:
- tokens: bfloat16 [1024, 2048], P(('dp', 'ep', 'tp'))
- expert_ids: int32 [1024, 8], P(('dp', 'ep', 'tp'))
- gates: float32 [1024, 8], P(('dp', 'ep', 'tp'))
- w_gate: bfloat16 [128, 2048, 768], P('ep', None, 'tp')
- w_up: bfloat16 [128, 2048, 768], P('ep', None, 'tp')
- w_down: bfloat16 [128, 768, 2048], P('ep', 'tp')
Outputs:
- output: bfloat16 [1024, 2048], P(('dp', 'ep', 'tp'))
All inputs are finite; a program needn't handle non-finite values.
Results may differ from the reference program's by a relative error of at most 0.0012.
Values are sent between devices in bfloat16 or wider.
A program may use at most 768 MiB of HBM per device.

```python
import jax
import jax.numpy as jnp
from jax import lax

TOKENS_DEV = 32
HIDDEN = 2048
EXPERT_FF = 768
EXPERTS = 128
TOP_K = 8
EP_SIZE = 8
TP_SIZE = 4

TOKENS = TOKENS_DEV * EP_SIZE * TP_SIZE
SPREAD = min(TOP_K, EP_SIZE)


def routing_ids(base_key):
    group_devices = EP_SIZE * TP_SIZE
    class_rows = TOKENS_DEV // EP_SIZE
    local_count = EXPERTS // EP_SIZE
    key_rows, key_target, key_rot = jax.random.split(base_key, 3)
    row_order = jax.vmap(lambda sub_key: jax.random.permutation(sub_key, TOKENS_DEV))(jax.random.split(key_rows, group_devices))
    ep_order = jax.vmap(lambda sub_key: jax.random.permutation(sub_key, EP_SIZE))(jax.random.split(key_target, group_devices))
    rotation = jax.random.randint(key_rot, (), 0, local_count)
    slots = jnp.arange(TOP_K)
    ep_class = row_order % EP_SIZE
    within = row_order // EP_SIZE + jnp.arange(group_devices)[:, None] * class_rows
    place = (ep_class[:, :, None] + slots % SPREAD) % EP_SIZE
    target_ep = jax.vmap(lambda order_row, place_rows: order_row[place_rows])(ep_order, place)
    local_slot = (within[:, :, None] + slots // SPREAD + rotation) % local_count
    return (target_ep * local_count + local_slot).astype(jnp.int32).reshape(TOKENS, TOP_K)


def setup_inputs(seed: int = 0, part: int = 0) -> dict:
    base_key = jax.random.key(seed)
    key_gate_w, key_up_w, key_down_w, key_part = jax.random.split(base_key, 4)
    key_tokens, key_ids, key_gates = jax.random.split(jax.random.fold_in(key_part, part), 3)
    tokens = jax.random.normal(key_tokens, (TOKENS, HIDDEN), jnp.float32).astype(jnp.bfloat16)
    expert_ids = routing_ids(key_ids)
    gates = jax.random.uniform(key_gates, (TOKENS, TOP_K), jnp.float32, 0.5, 1.5)
    w_gate = (jax.random.normal(key_gate_w, (EXPERTS, HIDDEN, EXPERT_FF), jnp.float32) * HIDDEN ** -0.5).astype(jnp.bfloat16)
    w_up = (jax.random.normal(key_up_w, (EXPERTS, HIDDEN, EXPERT_FF), jnp.float32) * HIDDEN ** -0.5).astype(jnp.bfloat16)
    w_down = (jax.random.normal(key_down_w, (EXPERTS, EXPERT_FF, HIDDEN), jnp.float32) * EXPERT_FF ** -0.5).astype(jnp.bfloat16)
    return {"tokens": tokens, "expert_ids": expert_ids, "gates": gates, "w_gate": w_gate, "w_up": w_up, "w_down": w_down}


def reference(tokens, expert_ids, gates, w_gate, w_up, w_down):
    load = TOKENS * TOP_K // EXPERTS
    order = jnp.argsort(expert_ids.reshape(-1), stable=True).reshape(EXPERTS, load)
    row_index = order // TOP_K
    gate_sorted = gates.reshape(-1)[order]

    def expert_out(operands):
        rows_in, gate_in, gate_mat, up_mat, down_mat = operands
        x_rows = tokens[rows_in]
        hidden_gate = jnp.dot(x_rows, gate_mat, preferred_element_type=jnp.float32)
        hidden_up = jnp.dot(x_rows, up_mat, preferred_element_type=jnp.float32)
        act_rows = (jax.nn.silu(hidden_gate) * hidden_up).astype(jnp.bfloat16)
        out_rows = jnp.dot(act_rows, down_mat, preferred_element_type=jnp.float32)
        return out_rows * gate_in[:, None]

    weighted = lax.map(expert_out, (row_index, gate_sorted, w_gate, w_up, w_down))
    summed = jax.ops.segment_sum(weighted.reshape(-1, HIDDEN), row_index.reshape(-1), num_segments=TOKENS)
    return summed.astype(jnp.bfloat16)
```

```python
import functools

import jax
import jax.numpy as jnp
from jax import lax
from jax.experimental import pallas as pl
from jax.experimental.pallas import tpu as pltpu
from jax.sharding import PartitionSpec as P

MESH = pl.DeviceIdType.MESH
BF = jnp.bfloat16
F32 = jnp.float32
CW = 256
WD_SLOTS = 4


def kernel(dims, tok, ids, gat, wg, wu, wd, out,
           xg, meta_src, meta, pmat, xs, wbuf, acc, h_t, lecol, gcol, hexp, wdbuf,
           part, d2d, mrec, nrec,
           ag_send, ag_recv, meta_send, meta_recv, w_sem, wd_sem, rs_send, rs_recv):
    nx, ny, ne, ff, rows, hid = dims
    nch = hid // CW
    group = 2 * nx * ny * rows
    plane = group // 2
    line = ny * rows
    load = group // ne
    ep_n = 2 * nx
    y = lax.axis_index("tp")
    ep = lax.axis_index("ep")
    x = ep // 2
    c = ep % 2
    o = 1 - c

    def dev(xx, yy, cc):
        return {"tp": yy, "ep": 2 * xx + cc}

    def xo(s):
        return lax.rem(x + (s + nx), nx)

    def yo(s):
        return lax.rem(y + (s + ny), ny)

    def w_copy(k, which):
        src = (wg, wu)[which]
        return pltpu.make_async_copy(src.at[:, :, pl.ds(k * CW, CW)],
                                     wbuf.at[k, :, pl.ds(which * ff, ff), :], w_sem.at[k, which])

    def wd_copy(j):
        return pltpu.make_async_copy(wd.at[:, pl.ds(j * CW, CW)], wdbuf.at[j % WD_SLOTS], wd_sem.at[j % WD_SLOTS])

    barrier = pltpu.get_barrier_semaphore()
    n_dev = ep_n * ny
    me = y * ep_n + ep

    def greet(i, carry):
        flat = lax.rem(me + i, n_dev)
        pl.semaphore_signal(barrier, inc=1, device_id={"tp": flat // ep_n, "ep": lax.rem(flat, ep_n)},
                            device_id_type=MESH)
        return carry

    lax.fori_loop(1, n_dev, greet, 0)

    for k in range(nch):
        for which in range(2):
            w_copy(k, which).start()
    for j in range(WD_SLOTS):
        wd_copy(j).start()

    ids4 = jnp.concatenate([ids[...]] * ny, axis=1)
    gat4 = jnp.concatenate([gat[...]] * ny, axis=1)
    lane = lax.broadcasted_iota(jnp.int32, (1, line), 1)
    mine = (lane // rows) == y
    for p in range(ep_n):
        sel = (ids4 // ne) == p
        le = jnp.sum(jnp.where(sel, ids4 - p * ne, 0).astype(F32), axis=0, keepdims=True)
        ga = jnp.sum(jnp.where(sel, gat4, 0.0), axis=0, keepdims=True)
        meta_src[p, :, pl.ds(0, line)] = jnp.where(mine, le, 0.0)
        meta_src[p, :, pl.ds(line, line)] = jnp.where(mine, ga, 0.0)
    my_block = (c * nx + x) * ny + y
    meta[my_block] = meta_src[ep]
    for k in range(nch):
        xg[k, c, x, y] = tok[:, pl.ds(k * CW, CW)]

    pl.semaphore_wait(barrier, n_dev - 1)

    def send_meta(i, carry):
        flat = lax.rem(me + i, n_dev)
        pe = lax.rem(flat, ep_n)
        pltpu.make_async_remote_copy(
            src_ref=meta_src.at[pe], dst_ref=meta.at[my_block], send_sem=meta_send, recv_sem=meta_recv,
            device_id={"tp": flat // ep_n, "ep": pe}, device_id_type=MESH).start()
        return carry

    lax.fori_loop(1, n_dev, send_meta, 0)

    def rcopy(k, kind, src, dst, to):
        return pltpu.make_async_remote_copy(src_ref=src, dst_ref=dst, send_sem=ag_send.at[k, kind],
                                            recv_sem=ag_recv.at[k, kind], device_id=to, device_id_type=MESH)

    def along(k, first, s):
        use_x = (k % 2 == 0) == first
        return dev(xo(s), y, c) if use_x else dev(x, yo(s), c)

    def block(k, s):
        return xg.at[k, c, xo(s), y] if k % 2 == 0 else xg.at[k, c, x, yo(s)]

    def lines(k, s, cc):
        return xg.at[k, cc, :, yo(s)] if k % 2 == 0 else xg.at[k, cc, xo(s)]

    def dirn(k):
        return 1 if (k // 2) % 2 == 0 else -1

    partner = dev(x, y, o)

    def a0(k):
        src = tok.at[:, pl.ds(k * CW, CW)]
        rcopy(k, 0, src, block(k, 0), along(k, True, 1)).start()
        rcopy(k, 1, src, block(k, 0), along(k, True, -1)).start()

    def wait(k, kind, dst):
        rcopy(k, kind, dst, dst, partner).wait_recv()

    def a1(k):
        d = dirn(k)
        first, second = (0, 1) if d == 1 else (1, 0)
        wait(k, first, block(k, -d))
        rcopy(k, 2, block(k, -d), block(k, -d), along(k, True, d)).start()
        wait(k, second, block(k, d))

    def a2(k):
        wait(k, 2, block(k, 2))
        rcopy(k, 3, lines(k, 0, c), lines(k, 0, c), along(k, False, 1)).start()
        rcopy(k, 4, lines(k, 0, c), lines(k, 0, c), along(k, False, -1)).start()
        rcopy(k, 6, lines(k, 0, c), lines(k, 0, c), partner).start()

    def a3(k):
        d = dirn(k)
        first, second = (3, 4) if d == 1 else (4, 3)
        wait(k, first, lines(k, -d, c))
        rcopy(k, 5, lines(k, -d, c), lines(k, -d, c), along(k, False, d)).start()
        rcopy(k, 7, lines(k, -d, c), lines(k, -d, c), partner).start()
        wait(k, second, lines(k, d, c))
        rcopy(k, 8, lines(k, d, c), lines(k, d, c), partner).start()

    def a4(k):
        wait(k, 5, lines(k, 2, c))
        rcopy(k, 9, lines(k, 2, c), lines(k, 2, c), partner).start()

    def a5(k):
        d = dirn(k)
        wait(k, 6, lines(k, 0, o))
        wait(k, 7, lines(k, -d, o))
        wait(k, 8, lines(k, d, o))
        wait(k, 9, lines(k, 2, o))

    n_grp = 2 * nx

    def build_perm():
        all_meta = meta.at[pl.ds(0, n_dev - 1)]
        pltpu.make_async_remote_copy(src_ref=all_meta, dst_ref=all_meta, send_sem=meta_send, recv_sem=meta_recv,
                                     device_id=partner, device_id_type=MESH).wait()
        les, gas = [], []
        for g in range(n_grp):
            row = meta[g * ny]
            for i in range(1, ny):
                row = row + meta[g * ny + i]
            les.append(row[:, :line])
            gas.append(row[:, line:])
        e_iota = lax.broadcasted_iota(jnp.int32, (ne, line), 0).astype(F32)
        hots = [jnp.where(e_iota == le, 1.0, 0.0) for le in les]
        r_i = lax.broadcasted_iota(jnp.int32, (line, line), 0)
        c_i = lax.broadcasted_iota(jnp.int32, (line, line), 1)
        upper = jnp.where(r_i < c_i, 1.0, 0.0).astype(BF)
        before = jnp.dot(jnp.concatenate(hots, axis=0).astype(BF), upper, preferred_element_type=F32)
        off = jnp.zeros((ne, 1), F32)
        s_iota = lax.broadcasted_iota(jnp.int32, (group, line), 0).astype(F32)
        for g in range(n_grp):
            pos = jnp.sum(hots[g] * (e_iota * load + off + before[g * ne:(g + 1) * ne]), axis=0, keepdims=True)
            off = off + jnp.sum(hots[g], axis=1, keepdims=True)
            pmat[:, pl.ds(g * line, line)] = jnp.where(s_iota == pos, 1.0, 0.0).astype(BF)
        le_t = jnp.concatenate(les, axis=0).T
        ga_t = jnp.concatenate(gas, axis=0).T
        for g in range(n_grp):
            lecol[pl.ds(g * line, line), :] = jnp.broadcast_to(le_t[:, g:g + 1], (line, 128))
            gcol[pl.ds(g * line, line), :] = jnp.broadcast_to(ga_t[:, g:g + 1], (line, 128))

    half_lane = lax.broadcasted_iota(jnp.int32, (2 * ff, 2 * load), 1) < load

    def compute(k):
        xk = xg.at[k].reshape(group, CW)

        def perm(m, carry):
            sl = pl.ds(pl.multiple_of(m * (group // 2), group // 2), group // 2)
            xs[sl, :] = jnp.dot(pmat[sl, :], xk[...], preferred_element_type=F32).astype(BF)
            return carry

        lax.fori_loop(0, 2, perm, 0)
        w_copy(k, 0).wait()
        w_copy(k, 1).wait()

        def pair(p, carry):
            rhs = xs[pl.ds(pl.multiple_of(p * 2 * load, 2 * load), 2 * load), :]
            dn = (((1,), (1,)), ((), ()))
            r0 = lax.dot_general(wbuf[k, 2 * p], rhs, dn, preferred_element_type=F32)
            r1 = lax.dot_general(wbuf[k, 2 * p + 1], rhs, dn, preferred_element_type=F32)
            r = jnp.where(half_lane, r0, r1)
            if k == 0:
                acc[p] = r
            else:
                acc[p] = acc[p] + r
            return carry

        lax.fori_loop(0, ne // 2, pair, 0)

    for k in range(nch):
        a0(k)
    lag = 5
    for t in range(nch + lag):
        if t < nch:
            a1(t)
        if 0 <= t - 1 < nch:
            a2(t - 1)
        if 0 <= t - 2 < nch:
            a3(t - 2)
        if 0 <= t - 3 < nch:
            a4(t - 3)
        if t == 3:
            build_perm()
        if 0 <= t - 5 < nch:
            a5(t - 5)
            compute(t - 5)

    for p in range(ne // 2):
        a = acc[p, :ff, :]
        b = acc[p, ff:, :]
        h_t[:, pl.ds(p * 2 * load, 2 * load)] = (jax.nn.silu(a) * b).astype(BF)
    wide = 4 * ff
    col_e = (lax.broadcasted_iota(jnp.int32, (line, wide), 1) // ff).astype(F32)

    def expand(g, carry):
        sl = pl.ds(pl.multiple_of(g * line, line), line)
        ht = jnp.dot(h_t[...], pmat[:, sl], preferred_element_type=F32)
        h = ht.T
        rep = jnp.concatenate([h] * 4, axis=1)
        le = jnp.broadcast_to(lecol[sl, :][:, :1], (line, wide))
        for q in range(ne // 4):
            hexp[sl, pl.ds(q * wide, wide)] = jnp.where(col_e + 4.0 * q == le, rep, 0.0).astype(BF)
        return carry

    lax.fori_loop(0, n_grp, expand, 0)

    def scopy(j, kind, src, dst, to):
        return pltpu.make_async_remote_copy(src_ref=src, dst_ref=dst, send_sem=rs_send.at[j, kind],
                                            recv_sem=rs_recv.at[j, kind], device_id=to, device_id_type=MESH)

    def down(j):
        slot = lax.rem(j, WD_SLOTS)
        pltpu.make_async_copy(wd.at[:, pl.ds(0, CW)], wdbuf.at[slot], wd_sem.at[slot]).wait()

        def one(i, carry):
            cc = jnp.where(i == 0, o, c)
            base = pl.multiple_of(cc * plane, plane)
            v = jnp.dot(hexp[pl.ds(base, plane), :], wdbuf[slot], preferred_element_type=F32)
            gt = gcol[pl.ds(base, plane), :]
            v = jnp.concatenate([v[:, q * 128:(q + 1) * 128] * gt for q in range(CW // 128)], axis=1)
            part[j, cc] = v.reshape(nx, ny, rows, CW)

            @pl.when(i == 0)
            def _():
                scopy(j, 0, part.at[j, o], d2d.at[j], partner).start()

            return carry

        lax.fori_loop(0, 2, one, 0)

        @pl.when(j + WD_SLOTS < nch)
        def _():
            pltpu.make_async_copy(wd.at[:, pl.ds(pl.multiple_of((j + WD_SLOTS) * CW, CW), CW)],
                                  wdbuf.at[slot], wd_sem.at[slot]).start()

    def stages(i, hf):
        j = 2 * i + hf
        d = 1 - 2 * lax.rem(i, 2)

        def xd(s):
            return lax.rem(x + s + 2 * nx, nx)

        def yd(s):
            return lax.rem(y + s + 2 * ny, ny)

        def big(s):
            return part.at[j, c, :, yd(s)] if hf == 0 else part.at[j, c, xd(s)]

        def big_to(s):
            return dev(x, yd(s), c) if hf == 0 else dev(xd(s), y, c)

        def small(s):
            return part.at[j, c, xd(s), y] if hf == 0 else part.at[j, c, x, yd(s)]

        def small_to(s):
            return dev(xd(s), y, c) if hf == 0 else dev(x, yd(s), c)

        def s1():
            scopy(j, 0, d2d.at[j], d2d.at[j], partner).wait_recv()
            part[j, c] = part[j, c] + d2d[j]
            scopy(j, 1, big(2), mrec.at[j, 0], big_to(d)).start()
            scopy(j, 2, big(-d), mrec.at[j, 1], big_to(-d)).start()

        def s2():
            scopy(j, 1, mrec.at[j, 0], mrec.at[j, 0], partner).wait_recv()
            big(d)[...] = big(d)[...] + mrec[j, 0]
            scopy(j, 3, big(d), mrec.at[j, 2], big_to(d)).start()

        def s3():
            scopy(j, 2, mrec.at[j, 1], mrec.at[j, 1], partner).wait_recv()
            scopy(j, 3, mrec.at[j, 2], mrec.at[j, 2], partner).wait_recv()
            big(0)[...] = big(0)[...] + mrec[j, 1] + mrec[j, 2]
            scopy(j, 4, small(2), nrec.at[j, 0], small_to(d)).start()
            scopy(j, 5, small(-d), nrec.at[j, 1], small_to(-d)).start()

        def s4():
            scopy(j, 4, nrec.at[j, 0], nrec.at[j, 0], partner).wait_recv()
            small(d)[...] = small(d)[...] + nrec[j, 0]
            scopy(j, 6, small(d), nrec.at[j, 2], small_to(d)).start()

        def s5():
            scopy(j, 5, nrec.at[j, 1], nrec.at[j, 1], partner).wait_recv()
            scopy(j, 6, nrec.at[j, 2], nrec.at[j, 2], partner).wait_recv()
            val = part[j, c, x, y] + nrec[j, 1] + nrec[j, 2]
            out[:, pl.ds(pl.multiple_of(j * CW, CW), CW)] = val.astype(BF)

        def sends():
            scopy(j, 0, part.at[j, o], d2d.at[j], partner).wait_send()
            scopy(j, 1, big(2), mrec.at[j, 0], partner).wait_send()
            scopy(j, 2, big(-d), mrec.at[j, 1], partner).wait_send()
            scopy(j, 3, big(d), mrec.at[j, 2], partner).wait_send()
            scopy(j, 4, small(2), nrec.at[j, 0], partner).wait_send()
            scopy(j, 5, small(-d), nrec.at[j, 1], partner).wait_send()
            scopy(j, 6, small(d), nrec.at[j, 2], partner).wait_send()

        return s1, s2, s3, s4, s5, sends

    half = nch // 2

    def rs_step(t, carry):
        for hf in range(2):
            @pl.when(t < half)
            def _():
                down(2 * t + hf)

            for n_s in range(1, 6):
                hf2 = (hf + n_s) % 2
                i = t + (hf - n_s - hf2) // 2

                @pl.when((i >= 0) & (i < half))
                def _():
                    stages(i, hf2)[n_s - 1]()
        return carry

    lax.fori_loop(0, (nch + 6) // 2, rs_step, 0)

    def fin(i, carry):
        for hf in range(2):
            stages(i, hf)[5]()
        return carry

    lax.fori_loop(0, half, fin, 0)
    for k in range(nch):
        for kind in range(3):
            src = block(k, 0)
            rcopy(k, kind, src, src, partner).wait_send()
        for kind in range(3, 10):
            rcopy(k, kind, lines(k, 0, c), lines(k, 0, c), partner).wait_send()


def solution(mesh):
    ep_n, ny = mesh.shape["ep"], mesh.shape["tp"]
    nx = ep_n // 2
    row_spec = P(("dp", "ep", "tp"), None)

    def layer(tokens, expert_ids, gates, w_gate, w_up, w_down):
        rows, hid = tokens.shape
        ne, ff, _ = w_down.shape
        group = rows * ep_n * ny
        nch = hid // CW
        dims = (nx, ny, ne, ff, rows, hid)
        vm = pl.BlockSpec(memory_space=pltpu.VMEM)
        hbm = pl.BlockSpec(memory_space=pl.ANY)
        dma = pltpu.SemaphoreType.DMA
        line = ny * rows
        scratch = [
            pltpu.VMEM((nch, 2, nx, ny, rows, CW), BF),
            pltpu.VMEM((ep_n, 1, 2 * line), F32),
            pltpu.VMEM((ep_n * ny, 1, 2 * line), F32),
            pltpu.VMEM((group, group), BF),
            pltpu.VMEM((group, CW), BF),
            pltpu.VMEM((nch, ne, 2 * ff, CW), BF),
            pltpu.VMEM((ne // 2, 2 * ff, 2 * (group // ne)), F32),
            pltpu.VMEM((ff, group), BF),
            pltpu.VMEM((group, 128), F32),
            pltpu.VMEM((group, 128), F32),
            pltpu.VMEM((group, ne * ff), BF),
            pltpu.VMEM((WD_SLOTS, ne * ff, CW), BF),
            pltpu.VMEM((nch, 2, nx, ny, rows, CW), F32),
            pltpu.VMEM((nch, nx, ny, rows, CW), F32),
            pltpu.VMEM((nch, 3, nx, rows, CW), F32),
            pltpu.VMEM((nch, 3, rows, CW), F32),
            dma((nch, 10)), dma((nch, 10)), dma, dma, dma((nch, 2)), dma((WD_SLOTS,)),
            dma((nch, 7)), dma((nch, 7)),
        ]
        return pl.pallas_call(
            functools.partial(kernel, dims),
            out_shape=jax.ShapeDtypeStruct((rows, hid), BF),
            in_specs=[vm, vm, vm, hbm, hbm, hbm],
            out_specs=vm,
            scratch_shapes=scratch,
            compiler_params=pltpu.CompilerParams(collective_id=0, has_side_effects=True,
                                                 vmem_limit_bytes=67_043_328),
        )(tokens, expert_ids.T, gates.T, jnp.swapaxes(w_gate, 1, 2), jnp.swapaxes(w_up, 1, 2),
          w_down.reshape(ne * ff, hid))

    w_spec = P("ep", None, "tp")
    return jax.shard_map(layer, mesh=mesh, in_specs=(row_spec, row_spec, row_spec, w_spec, w_spec, P("ep", "tp", None)),
                         out_specs=row_spec, check_vma=False)
```

```python
import functools

import jax
import jax.numpy as jnp
from jax import lax
from jax.experimental import pallas as pl
from jax.experimental.pallas import tpu as pltpu
from jax.sharding import PartitionSpec as P

MESH = pl.DeviceIdType.MESH
BF = jnp.bfloat16
F32 = jnp.float32
CW = 256
WD_SLOTS = 4
AG_LAGS = (0, 2, 4, 6, 7, 7)
PERM_AT = 4
RS_LAGS = (1, 3, 5, 7, 9)


def kernel(dims, tok, ids, gat, wg, wu, wd, out,
           xg, meta_src, meta, pmat, xs, wbuf, acc, h_t, lecol, gcol, hexp, wdbuf,
           part, d2d, mrec, nrec,
           ag_send, ag_recv, meta_send, meta_recv, w_sem, wd_sem, rs_send, rs_recv):
    nx, ny, ne, ff, rows, hid = dims
    nch = hid // CW
    group = 2 * nx * ny * rows
    plane = group // 2
    line = ny * rows
    load = group // ne
    ep_n = 2 * nx
    y = lax.axis_index("tp")
    ep = lax.axis_index("ep")
    x = ep // 2
    c = ep % 2
    o = 1 - c

    def dev(xx, yy, cc):
        return {"tp": yy, "ep": 2 * xx + cc}

    def xo(s):
        return lax.rem(x + s + 2 * nx, nx)

    def yo(s):
        return lax.rem(y + s + 2 * ny, ny)

    def w_copy(k, which):
        src = (wg, wu)[which]
        return pltpu.make_async_copy(src.at[:, :, pl.ds(pl.multiple_of(k * CW, CW) if not isinstance(k, int) else k * CW, CW)],
                                     wbuf.at[k, :, pl.ds(which * ff, ff), :], w_sem.at[k])

    def wd_copy(j):
        return pltpu.make_async_copy(wd.at[:, pl.ds(j * CW, CW)], wdbuf.at[j % WD_SLOTS], wd_sem.at[j % WD_SLOTS])

    barrier = pltpu.get_barrier_semaphore()
    n_dev = ep_n * ny
    me = y * ep_n + ep

    def greet(i, carry):
        flat = lax.rem(me + i, n_dev)
        pl.semaphore_signal(barrier, inc=1, device_id={"tp": flat // ep_n, "ep": lax.rem(flat, ep_n)},
                            device_id_type=MESH)
        return carry

    with jax.named_scope("greet"):
        lax.fori_loop(1, n_dev, greet, 0)

    with jax.named_scope("w_issue"):
        for k in range(nch):
            for which in range(2):
                w_copy(k, which).start()
        for j in range(WD_SLOTS):
            wd_copy(j).start()

    ids4 = jnp.concatenate([ids[...]] * ny, axis=1)
    gat4 = jnp.concatenate([gat[...]] * ny, axis=1)
    lane = lax.broadcasted_iota(jnp.int32, (1, line), 1)
    mine = (lane // rows) == y
    for p in range(ep_n):
        sel = (ids4 // ne) == p
        le = jnp.sum(jnp.where(sel, ids4 - p * ne, 0).astype(F32), axis=0, keepdims=True)
        ga = jnp.sum(jnp.where(sel, gat4, 0.0), axis=0, keepdims=True)
        meta_src[p, :, pl.ds(0, line)] = jnp.where(mine, le, 0.0)
        meta_src[p, :, pl.ds(line, line)] = jnp.where(mine, ga, 0.0)
    my_block = (c * nx + x) * ny + y
    meta[my_block] = meta_src[ep]
    for k in range(nch):
        xg[k, c, x, y] = tok[:, pl.ds(k * CW, CW)]

    acc[...] = jnp.zeros_like(acc)
    with jax.named_scope("barrier"):
        pl.semaphore_wait(barrier, n_dev - 1)

    def send_meta(i, carry):
        flat = lax.rem(me + i, n_dev)
        pe = lax.rem(flat, ep_n)
        pltpu.make_async_remote_copy(
            src_ref=meta_src.at[pe], dst_ref=meta.at[my_block], send_sem=meta_send, recv_sem=meta_recv,
            device_id={"tp": flat // ep_n, "ep": pe}, device_id_type=MESH).start()
        return carry

    lax.fori_loop(1, n_dev, send_meta, 0)

    partner = dev(x, y, o)

    def gather(i, hf):
        k = 2 * i + hf
        d = 1 - 2 * lax.rem(i, 2)

        def first_to(s):
            return dev(xo(s), y, c) if hf == 0 else dev(x, yo(s), c)

        def second_to(s):
            return dev(x, yo(s), c) if hf == 0 else dev(xo(s), y, c)

        def block(s):
            return xg.at[k, c, xo(s), y] if hf == 0 else xg.at[k, c, x, yo(s)]

        def lines(s, cc):
            return xg.at[k, cc, :, yo(s)] if hf == 0 else xg.at[k, cc, xo(s)]

        def rcopy(kind, src, dst, to):
            return pltpu.make_async_remote_copy(src_ref=src, dst_ref=dst, send_sem=ag_send,
                                                recv_sem=ag_recv.at[k, min(kind, 6) if isinstance(kind, int) else kind], device_id=to, device_id_type=MESH)

        def wait(kind, dst):
            rcopy(kind, dst, dst, partner).wait_recv()

        def a0():
            src = tok.at[:, pl.ds(pl.multiple_of(k * CW, CW), CW)]
            rcopy(0, src, block(0), first_to(1)).start()
            rcopy(1, src, block(0), first_to(-1)).start()

        def a1():
            back = jnp.where(d == 1, 0, 1)
            wait(back, block(-d))
            rcopy(2, block(-d), block(-d), first_to(d)).start()
            wait(1 - back, block(d))

        def a2():
            wait(2, block(2))
            rcopy(3, lines(0, c), lines(0, c), second_to(1)).start()
            rcopy(4, lines(0, c), lines(0, c), second_to(-1)).start()
            rcopy(6, lines(0, c), lines(0, c), partner).start()

        def a3():
            back = jnp.where(d == 1, 3, 4)
            wait(back, lines(-d, c))
            rcopy(5, lines(-d, c), lines(-d, c), second_to(d)).start()
            rcopy(7, lines(-d, c), lines(-d, c), partner).start()
            wait(7 - back, lines(d, c))
            rcopy(8, lines(d, c), lines(d, c), partner).start()

        def a4():
            wait(5, lines(2, c))
            rcopy(9, lines(2, c), lines(2, c), partner).start()

        def a5():
            wait(6, xg.at[k, o])

        return a0, a1, a2, a3, a4, a5

    n_grp = 2 * nx

    def build_perm():
        all_meta = meta.at[pl.ds(0, n_dev - 1)]
        pltpu.make_async_remote_copy(src_ref=all_meta, dst_ref=all_meta, send_sem=meta_send, recv_sem=meta_recv,
                                     device_id=partner, device_id_type=MESH).wait()
        les, gas = [], []
        for g in range(n_grp):
            row = meta[g * ny]
            for i in range(1, ny):
                row = row + meta[g * ny + i]
            les.append(row[:, :line])
            gas.append(row[:, line:])
        e_iota = lax.broadcasted_iota(jnp.int32, (ne, line), 0).astype(F32)
        hots = [jnp.where(e_iota == le, 1.0, 0.0) for le in les]
        r_i = lax.broadcasted_iota(jnp.int32, (line, line), 0)
        c_i = lax.broadcasted_iota(jnp.int32, (line, line), 1)
        upper = jnp.where(r_i < c_i, 1.0, 0.0).astype(BF)
        before = jnp.dot(jnp.concatenate(hots, axis=0).astype(BF), upper, preferred_element_type=F32)
        off = jnp.zeros((ne, 1), F32)
        s_iota = lax.broadcasted_iota(jnp.int32, (group, line), 0).astype(F32)
        for g in range(n_grp):
            pos = jnp.sum(hots[g] * (e_iota * load + off + before[g * ne:(g + 1) * ne]), axis=0, keepdims=True)
            off = off + jnp.sum(hots[g], axis=1, keepdims=True)
            pmat[:, pl.ds(g * line, line)] = jnp.where(s_iota == pos, 1.0, 0.0).astype(BF)
        le_t = jnp.concatenate(les, axis=0).T
        ga_t = jnp.concatenate(gas, axis=0).T
        for g in range(n_grp):
            lecol[pl.ds(g * line, line), :] = jnp.broadcast_to(le_t[:, g:g + 1], (line, 128)).astype(BF)
            gcol[pl.ds(g * line, line), :] = jnp.broadcast_to(ga_t[:, g:g + 1], (line, 128))

    half_lane = lax.broadcasted_iota(jnp.int32, (2 * ff, 2 * load), 1) < load

    def compute(k):
        xk = xg.at[k].reshape(group, CW)
        with jax.named_scope("perm"):
            for m in range(2):
                sl = pl.ds(m * (group // 2), group // 2)
                xs[sl, :] = jnp.dot(pmat[sl, :], xk[...], preferred_element_type=F32).astype(BF)
        pltpu.make_async_copy(wbuf.at[k], wbuf.at[k], w_sem.at[k]).wait()
        dn = (((1,), (1,)), ((), ()))
        with jax.named_scope("pairs"):
            for p in range(ne // 2):
                rhs = xs[pl.ds(p * 2 * load, 2 * load), :]
                r0 = lax.dot_general(wbuf[k, 2 * p], rhs, dn, preferred_element_type=F32)
                r1 = lax.dot_general(wbuf[k, 2 * p + 1], rhs, dn, preferred_element_type=F32)
                acc[p] = acc[p] + jnp.where(half_lane, r0, r1)

    half = nch // 2

    def each(fn):
        def go(i, carry):
            for hf in range(2):
                fn(i, hf)
            return carry
        lax.fori_loop(0, half, go, 0)

    def pipeline(stages, first, last):
        def go(t, carry):
            for hf in range(2):
                for lag, name, fn in stages:
                    hf2 = (hf + lag) % 2
                    i = t + (hf - lag - hf2) // 2

                    @pl.when((i >= 0) & (i < half))
                    def _():
                        with jax.named_scope(name):
                            fn(i, hf2)
            return carry
        lax.fori_loop(first // 2, last // 2, go, 0)

    with jax.named_scope("a0"):
        each(lambda i, hf: gather(i, hf)[0]())
    ag = [(lag, f"ag{n}", lambda i, hf, n=n: gather(i, hf)[n]()) for n, lag in enumerate(AG_LAGS[:5], 1)]
    ag.append((AG_LAGS[5], "compute", lambda i, hf: compute(2 * i + hf)))
    pipeline(ag, 0, PERM_AT)
    with jax.named_scope("build_perm"):
        build_perm()
    pipeline(ag, PERM_AT, (nch + max(AG_LAGS) + 1) // 2 * 2)

    with jax.named_scope("silu"):
        for p in range(ne // 2):
            a = acc[p, :ff, :]
            b = acc[p, ff:, :]
            h_t[:, pl.ds(p * 2 * load, 2 * load)] = (jax.nn.silu(a) * b).astype(BF)
    wide = 4 * ff

    def expand(cc):
        col_e = (lax.broadcasted_iota(jnp.int32, (line, wide), 1) // ff).astype(BF)
        ht = jnp.dot(h_t[...], pmat[:, pl.ds(pl.multiple_of(cc * plane, plane), plane)], preferred_element_type=F32)
        for g in range(plane // line):
            sl = pl.ds(pl.multiple_of(cc * plane + g * line, line), line)
            h = ht[:, g * line:(g + 1) * line].T.astype(BF)
            rep = jnp.concatenate([h] * 4, axis=1)
            le = jnp.concatenate([lecol[sl, :]] * (wide // 128), axis=1)
            for q in range(ne // 4):
                hexp[sl, pl.ds(q * wide, wide)] = jnp.where(col_e + BF(4 * q) == le, rep, BF(0))

    def scopy(j, kind, src, dst, to):
        return pltpu.make_async_remote_copy(src_ref=src, dst_ref=dst, send_sem=rs_send,
                                            recv_sem=rs_recv.at[j, kind], device_id=to, device_id_type=MESH)

    def down_half(j, slot, i):
        cc = jnp.where(i == 0, o, c)
        base = pl.multiple_of(cc * plane, plane)
        v = jnp.dot(hexp[pl.ds(base, plane), :], wdbuf[slot], preferred_element_type=F32)
        gt = gcol[pl.ds(base, plane), :]
        v = jnp.concatenate([v[:, q * 128:(q + 1) * 128] * gt for q in range(CW // 128)], axis=1)
        part[j, cc] = v.reshape(nx, ny, rows, CW)

        @pl.when(i == 0)
        def _():
            scopy(j, 0, part.at[j, o], d2d.at[j], partner).start()

    def down(j):
        slot = lax.rem(j, WD_SLOTS)
        pltpu.make_async_copy(wd.at[:, pl.ds(0, CW)], wdbuf.at[slot], wd_sem.at[slot]).wait()

        def one(i, carry):
            @pl.when(j == 0)
            def _():
                with jax.named_scope("expand"):
                    expand(jnp.where(i == 0, o, c))
            with jax.named_scope("half"):
                down_half(j, slot, i)
            return carry

        lax.fori_loop(0, 2, one, 0)

        @pl.when(j + WD_SLOTS < nch)
        def _():
            pltpu.make_async_copy(wd.at[:, pl.ds(pl.multiple_of((j + WD_SLOTS) * CW, CW), CW)],
                                  wdbuf.at[slot], wd_sem.at[slot]).start()

    def stages(i, hf):
        j = 2 * i + hf
        d = 1 - 2 * lax.rem(i, 2)

        def xd(s):
            return lax.rem(x + s + 2 * nx, nx)

        def yd(s):
            return lax.rem(y + s + 2 * ny, ny)

        def big(s):
            return part.at[j, c, :, yd(s)] if hf == 0 else part.at[j, c, xd(s)]

        def big_to(s):
            return dev(x, yd(s), c) if hf == 0 else dev(xd(s), y, c)

        def small(s):
            return part.at[j, c, xd(s), y] if hf == 0 else part.at[j, c, x, yd(s)]

        def small_to(s):
            return dev(xd(s), y, c) if hf == 0 else dev(x, yd(s), c)

        def s1():
            scopy(j, 0, d2d.at[j], d2d.at[j], partner).wait_recv()
            part[j, c] = part[j, c] + d2d[j]
            scopy(j, 1, big(2), mrec.at[j, 0], big_to(d)).start()
            scopy(j, 2, big(-d), mrec.at[j, 1], big_to(-d)).start()

        def s2():
            scopy(j, 1, mrec.at[j, 0], mrec.at[j, 0], partner).wait_recv()
            big(d)[...] = big(d)[...] + mrec[j, 0]
            scopy(j, 2, big(d), mrec.at[j, 2], big_to(d)).start()

        def s3():
            scopy(j, 2, mrec.at[j, pl.ds(1, 2)], mrec.at[j, pl.ds(1, 2)], partner).wait_recv()
            big(0)[...] = big(0)[...] + mrec[j, 1] + mrec[j, 2]
            scopy(j, 3, small(2), nrec.at[j, 0], small_to(d)).start()
            scopy(j, 4, small(-d), nrec.at[j, 1], small_to(-d)).start()

        def s4():
            scopy(j, 3, nrec.at[j, 0], nrec.at[j, 0], partner).wait_recv()
            small(d)[...] = small(d)[...] + nrec[j, 0]
            scopy(j, 4, small(d), nrec.at[j, 2], small_to(d)).start()

        def s5():
            scopy(j, 4, nrec.at[j, pl.ds(1, 2)], nrec.at[j, pl.ds(1, 2)], partner).wait_recv()
            val = part[j, c, x, y] + nrec[j, 1] + nrec[j, 2]
            out[:, pl.ds(pl.multiple_of(j * CW, CW), CW)] = val.astype(BF)

        return s1, s2, s3, s4, s5

    rs = [(0, "down", lambda i, hf: down(2 * i + hf))]
    rs += [(lag, f"rs{n}", lambda i, hf, n=n: stages(i, hf)[n - 1]()) for n, lag in enumerate(RS_LAGS, 1)]
    pipeline(rs, 0, (nch + max(RS_LAGS) + 1) // 2 * 2)
    with jax.named_scope("fin"):
        blocks = nch * (3 + 7 * nx)
        for buf, sem in ((xg, ag_send), (part, rs_send)):
            flat = buf.reshape(nch * 2 * nx * ny, rows, CW).at[pl.ds(0, blocks)]
            pltpu.make_async_remote_copy(src_ref=flat, dst_ref=flat, send_sem=sem, recv_sem=sem,
                                         device_id=partner, device_id_type=MESH).wait_send()


def solution(mesh):
    ep_n, ny = mesh.shape["ep"], mesh.shape["tp"]
    nx = ep_n // 2
    row_spec = P(("dp", "ep", "tp"), None)

    def layer(tokens, expert_ids, gates, w_gate, w_up, w_down):
        rows, hid = tokens.shape
        ne, ff, _ = w_down.shape
        group = rows * ep_n * ny
        nch = hid // CW
        dims = (nx, ny, ne, ff, rows, hid)
        vm = pl.BlockSpec(memory_space=pltpu.VMEM)
        hbm = pl.BlockSpec(memory_space=pl.ANY)
        dma = pltpu.SemaphoreType.DMA
        line = ny * rows
        scratch = [
            pltpu.VMEM((nch, 2, nx, ny, rows, CW), BF),
            pltpu.VMEM((ep_n, 1, 2 * line), F32),
            pltpu.VMEM((ep_n * ny, 1, 2 * line), F32),
            pltpu.VMEM((group, group), BF),
            pltpu.VMEM((group, CW), BF),
            pltpu.VMEM((nch, ne, 2 * ff, CW), BF),
            pltpu.VMEM((ne // 2, 2 * ff, 2 * (group // ne)), F32),
            pltpu.VMEM((ff, group), BF),
            pltpu.VMEM((group, 128), BF),
            pltpu.VMEM((group, 128), F32),
            pltpu.VMEM((group, ne * ff), BF),
            pltpu.VMEM((WD_SLOTS, ne * ff, CW), BF),
            pltpu.VMEM((nch, 2, nx, ny, rows, CW), F32),
            pltpu.VMEM((nch, nx, ny, rows, CW), F32),
            pltpu.VMEM((nch, 3, nx, rows, CW), F32),
            pltpu.VMEM((nch, 3, rows, CW), F32),
            dma, dma((nch, 7)), dma, dma, dma((nch,)), dma((WD_SLOTS,)),
            dma, dma((nch, 5)),
        ]
        return pl.pallas_call(
            functools.partial(kernel, dims),
            out_shape=jax.ShapeDtypeStruct((rows, hid), BF),
            in_specs=[vm, vm, vm, hbm, hbm, hbm],
            out_specs=vm,
            scratch_shapes=scratch,
            compiler_params=pltpu.CompilerParams(collective_id=0, has_side_effects=True,
                                                 vmem_limit_bytes=67_043_328),
        )(tokens, expert_ids.T, gates.T, jnp.swapaxes(w_gate, 1, 2), jnp.swapaxes(w_up, 1, 2),
          w_down.reshape(ne * ff, hid))

    w_spec = P("ep", None, "tp")
    return jax.shard_map(layer, mesh=mesh, in_specs=(row_spec, row_spec, row_spec, w_spec, w_spec, P("ep", "tp", None)),
                         out_specs=row_spec, check_vma=False)
```

```python
import functools

import jax
import jax.numpy as jnp
from jax import lax
from jax.experimental import pallas as pl
from jax.experimental.pallas import tpu as pltpu
from jax.sharding import PartitionSpec as P

MESH = pl.DeviceIdType.MESH
BF = jnp.bfloat16
F32 = jnp.float32
CW = 256
WD_SLOTS = 3
N_DIRECT = 3
DIRECT = 0
FILL = ("0.0", "0.1", "0.2", "0.3", "0.4", "0.5", "0.6", "0.7", "m1", "1.0", "1.1", "1.2", "1.3", "m2", "2.0", "2.1",
        "1.4", "1.5", "b", "2.2", "2.3", "3.0", "3.1", "1.6", "1.7")
RS_LAGS = (1, 3, 5, 8, 10)
M2_LATE = 8


def kernel(dims, tok_hbm, ids_hbm, gat_hbm, wg, wu, wd, out,
           tok, ids, gat, in_sem, xg, meta_src, meta, pmat, xs, wbuf, acc, h_t, lecol, gcol, hexp, wdbuf,
           part, d2d, mrec, nrec,
           ag_send, ag_recv, meta_send, meta_recv, w_sem, wd_sem, rs_send, rs_recv):
    nx, ny, ne, ff, rows, hid = dims
    nch = hid // CW
    group = 2 * nx * ny * rows
    plane = group // 2
    line = ny * rows
    load = group // ne
    ep_n = 2 * nx
    y = lax.axis_index("tp")
    ep = lax.axis_index("ep")
    x = ep // 2
    c = ep % 2
    o = 1 - c

    def dev(xx, yy, cc):
        return {"tp": yy, "ep": 2 * xx + cc}

    def xo(s):
        return lax.rem(x + s + 2 * nx, nx)

    def yo(s):
        return lax.rem(y + s + 2 * ny, ny)

    def w_copy(k, which):
        src = (wg, wu)[which]
        return pltpu.make_async_copy(src.at[:, :, pl.ds(pl.multiple_of(k * CW, CW) if not isinstance(k, int) else k * CW, CW)],
                                     wbuf.at[k, :, pl.ds(which * ff, ff), :], w_sem.at[k])

    def wd_copy(j):
        return pltpu.make_async_copy(wd.at[:, pl.ds(j * CW, CW)], wdbuf.at[j % WD_SLOTS], wd_sem.at[j % WD_SLOTS])

    barrier = pltpu.get_barrier_semaphore()
    peers = [dev(xo(i), y, c) for i in range(1, nx)] + [dev(x, yo(i), c) for i in range(1, ny)] + [dev(x, y, o)]
    for peer in peers:
        pl.semaphore_signal(barrier, inc=1, device_id=peer, device_id_type=MESH)

    own = [pltpu.make_async_copy(src, dst, in_sem.at[n])
           for n, (src, dst) in enumerate(((ids_hbm, ids), (gat_hbm, gat), (tok_hbm, tok)))]
    for copy in own:
        copy.start()
    with jax.named_scope("w_issue"):
        for k in range(nch):
            for which in range(2):
                w_copy(k, which).start()
        for j in range(WD_SLOTS):
            wd_copy(j).start()

    own[0].wait()
    own[1].wait()
    ids4 = jnp.concatenate([ids[...]] * ny, axis=1)
    gat4 = jnp.concatenate([gat[...]] * ny, axis=1)
    lane = lax.broadcasted_iota(jnp.int32, (1, line), 1)
    mine = (lane // rows) == y
    for p in range(ep_n):
        sel = (ids4 // ne) == p
        le = jnp.sum(jnp.where(sel, ids4 - p * ne, 0).astype(F32), axis=0, keepdims=True)
        ga = jnp.sum(jnp.where(sel, gat4, 0.0), axis=0, keepdims=True)
        meta_src[p, :, pl.ds(0, line)] = jnp.where(mine, le, 0.0)
        meta_src[p, :, pl.ds(line, line)] = jnp.where(mine, ga, 0.0)
    for e2 in range(2):
        meta[c, x, y, e2] = meta_src[2 * x + e2]
    own[2].wait()
    for k in range(nch):
        xg[k, c, x, y] = tok[:, pl.ds(k * CW, CW)]

    acc[...] = jnp.zeros_like(acc)
    with jax.named_scope("barrier"):
        pl.semaphore_wait(barrier, len(peers))

    def mcopy(n, src, dst, to):
        return pltpu.make_async_remote_copy(src_ref=src, dst_ref=dst, send_sem=meta_send.at[n], recv_sem=meta_recv.at[n],
                                            device_id=to, device_id_type=MESH)

    def meta0():
        for i in range(1, nx):
            mcopy(0, meta_src.at[pl.ds(2 * xo(i), 2)], meta.at[c, x, y], dev(xo(i), y, c)).start()

    def meta1():
        whole = meta_src.at[pl.ds(0, 2 * (nx - 1))]
        mcopy(0, whole, whole, dev(x, y, o)).wait()
        for i in range(1, ny):
            mcopy(1, meta.at[c, :, y], meta.at[c, :, y], dev(x, yo(i), c)).start()

    def meta2():
        whole = meta.at[c, :, pl.ds(0, ny - 1)]
        mcopy(1, whole, whole, dev(x, y, o)).wait()
        mcopy(2, meta.at[c], meta.at[c], dev(x, y, o)).start()

    partner = dev(x, y, o)
    hw = CW // 2

    def gather(i, hf, direct=False):
        k = 2 * i + hf

        def first_to(s):
            return dev(xo(s), y, c) if hf == 0 else dev(x, yo(s), c)

        def second_to(s):
            return dev(x, yo(s), c) if hf == 0 else dev(xo(s), y, c)

        def block(s):
            return xg.at[k, c, xo(s), y] if hf == 0 else xg.at[k, c, x, yo(s)]

        def lines(s, cc, sub=slice(None)):
            return xg.at[k, cc, sub, yo(s)] if hf == 0 else xg.at[k, cc, xo(s), sub]

        def rcopy(kind, ref, to, src=None):
            return pltpu.make_async_remote_copy(src_ref=ref if src is None else src, dst_ref=ref, send_sem=ag_send,
                                                recv_sem=ag_recv.at[k, kind], device_id=to, device_id_type=MESH)

        def a0():
            src = tok.at[:, pl.ds(pl.multiple_of(k * CW, CW), CW)]
            for s in (1, -1, 2):
                rcopy(0, block(0), first_to(s), src).start()

        def a1():
            rcopy(0, xg.at[k, c, 0, pl.ds(0, 3)], partner).wait_recv()
            rcopy(1, lines(0, c), second_to(1)).start()
            rcopy(2, lines(0, c), second_to(-1)).start()
            if direct:
                rcopy(3, lines(0, c), second_to(2)).start()
            rcopy(4, lines(0, c), partner).start()

        def a2():
            for n, s in ((1, -1), (2, 1)):
                rcopy(n, lines(s, c), partner).wait_recv()
                if not direct:
                    rcopy(3, lines(s, c, pl.ds((n - 1) * (nx // 2), nx // 2)), second_to(-s)).start()
                rcopy(4, lines(s, c), partner).start()

        def a3():
            rcopy(3, lines(2, c), partner).wait_recv()
            rcopy(4, lines(2, c), partner).start()

        def a4():
            rcopy(4, xg.at[k, o], partner).wait_recv()

        return a0, a1, a2, a3, a4

    n_grp = 2 * nx

    def build_perm():
        mcopy(2, meta.at[c], meta.at[o], dev(x, y, o)).wait()
        les, gas = [], []
        for g in range(n_grp):
            row = meta[g // nx, g % nx, 0, c]
            for i in range(1, ny):
                row = row + meta[g // nx, g % nx, i, c]
            les.append(row[:, :line])
            gas.append(row[:, line:])
        e_iota = lax.broadcasted_iota(jnp.int32, (ne, line), 0).astype(F32)
        hots = [jnp.where(e_iota == le, 1.0, 0.0) for le in les]
        r_i = lax.broadcasted_iota(jnp.int32, (line, line), 0)
        c_i = lax.broadcasted_iota(jnp.int32, (line, line), 1)
        upper = jnp.where(r_i < c_i, 1.0, 0.0).astype(BF)
        before = jnp.dot(jnp.concatenate(hots, axis=0).astype(BF), upper, preferred_element_type=F32)
        off = jnp.zeros((ne, 1), F32)
        s_iota = lax.broadcasted_iota(jnp.int32, (group, line), 0).astype(F32)
        for g in range(n_grp):
            pos = jnp.sum(hots[g] * (e_iota * load + off + before[g * ne:(g + 1) * ne]), axis=0, keepdims=True)
            off = off + jnp.sum(hots[g], axis=1, keepdims=True)
            pmat[:, pl.ds(g * line, line)] = jnp.where(s_iota == pos, 1.0, 0.0).astype(BF)
        le_t = jnp.concatenate(les, axis=0).T
        ga_t = jnp.concatenate(gas, axis=0).T
        for g in range(n_grp):
            lecol[pl.ds(g * line, line), :] = jnp.broadcast_to(le_t[:, g:g + 1], (line, 128)).astype(BF)
            gcol[pl.ds(g * line, line), :] = jnp.broadcast_to(ga_t[:, g:g + 1], (line, 128))

    half_lane = lax.broadcasted_iota(jnp.int32, (2 * ff, 2 * load), 1) < load

    def compute(k):
        xk = xg.at[k].reshape(group, CW)
        with jax.named_scope("perm"):
            for m in range(2):
                sl = pl.ds(m * (group // 2), group // 2)
                xs[sl, :] = jnp.dot(pmat[sl, :], xk[...], preferred_element_type=F32).astype(BF)
        pltpu.make_async_copy(wbuf.at[k], wbuf.at[k], w_sem.at[k]).wait()
        dn = (((1,), (1,)), ((), ()))
        with jax.named_scope("pairs"):
            for p in range(ne // 2):
                rhs = xs[pl.ds(p * 2 * load, 2 * load), :]
                both = wbuf[k, pl.ds(2 * p, 2)].reshape(4 * ff, CW)
                r = lax.dot_general(both, rhs, dn, preferred_element_type=F32)
                acc[p] = acc[p] + jnp.where(half_lane, r[:2 * ff], r[2 * ff:])

    half = nch // 2

    meta0()
    done = [0] * 5
    for event in FILL:
        with jax.named_scope(event):
            if event in ("m1", "m2", "b"):
                {"m1": meta1, "m2": meta2, "b": build_perm}[event]()
            else:
                n, k = (int(v) for v in event.split("."))
                gather(k // 2, k % 2, k < DIRECT)[n]()
                done[n] = k + 1
    assert done[0] == nch

    def steady(i, carry):
        for hf in range(2):
            with jax.named_scope("ag4"):
                gather(i, hf)[4]()
            with jax.named_scope("compute"):
                compute(2 * i + hf)
            for n in range(1, 4):
                hf2 = (hf + done[n]) % 2
                ii = i + (hf + done[n] - hf2) // 2

                @pl.when(ii < half)
                def _():
                    with jax.named_scope(f"ag{n}"):
                        gather(ii, hf2)[n]()
        return carry

    lax.fori_loop(0, half, steady, 0)

    with jax.named_scope("silu"):
        for p in range(ne // 2):
            a = acc[p, :ff, :]
            b = acc[p, ff:, :]
            h_t[:, pl.ds(p * 2 * load, 2 * load)] = (jax.nn.silu(a) * b).astype(BF)
    wide = 4 * ff

    def expand(cc):
        col_e = (lax.broadcasted_iota(jnp.int32, (line, wide), 1) // ff).astype(BF)
        ht = jnp.dot(h_t[...], pmat[:, pl.ds(pl.multiple_of(cc * plane, plane), plane)], preferred_element_type=F32)
        for g in range(plane // line):
            sl = pl.ds(pl.multiple_of(cc * plane + g * line, line), line)
            h = ht[:, g * line:(g + 1) * line].T.astype(BF)
            rep = jnp.concatenate([h] * 4, axis=1)
            le = jnp.concatenate([lecol[sl, :]] * (wide // 128), axis=1)
            for q in range(ne // 4):
                hexp[sl, pl.ds(q * wide, wide)] = jnp.where(col_e + BF(4 * q) == le, rep, BF(0))

    def scopy(j, kind, src, dst, to):
        return pltpu.make_async_remote_copy(src_ref=src, dst_ref=dst, send_sem=rs_send,
                                            recv_sem=rs_recv.at[j, kind], device_id=to, device_id_type=MESH)

    def down_half(j, cc):
        base = pl.multiple_of(cc * plane, plane)

        @pl.when(j == 0)
        def _():
            with jax.named_scope("expand"):
                expand(cc)

        with jax.named_scope("half"):
            v = jnp.dot(hexp[pl.ds(base, plane), :], wdbuf[lax.rem(j, WD_SLOTS)], preferred_element_type=F32)
            gt = gcol[pl.ds(base, plane), :]
            for h in range(2):
                part[j, cc, h] = (v[:, h * hw:(h + 1) * hw] * gt).reshape(nx, ny, rows, hw)

    def wd_next(j):
        slot = lax.rem(j, WD_SLOTS)
        return pltpu.make_async_copy(wd.at[:, pl.ds(pl.multiple_of(j * CW, CW), CW)], wdbuf.at[slot], wd_sem.at[slot])

    def stages(j):
        ways = ((0, 1), (1, -1))
        q_rows = rows // 2

        def big(h, s, sub=slice(None)):
            return part.at[j, c, h, sub, yo(s)] if h == 0 else part.at[j, c, h, xo(s), sub]

        def small(h, s, sub=slice(None)):
            return part.at[j, c, h, xo(s), y, sub] if h == 0 else part.at[j, c, h, x, yo(s), sub]

        def to(along_y, s):
            return dev(x, yo(s), c) if along_y else dev(xo(s), y, c)

        def direct(part_of, rec, n, first, sem):
            for h in range(2):
                for q, s in ways:
                    sub = pl.ds((1 - q) * n, n)
                    scopy(j, sem + 1, part_of(h, s, sub), rec.at[j, h, 1 + q, sub], to((h == 0) == first, s)).start()

        def begin(part_of, rec, n, first, sem):
            for h in range(2):
                for q, s in ways:
                    sub = pl.ds(q * n, n)
                    scopy(j, sem, part_of(h, 2, sub), rec.at[j, h, 0, sub], to((h == 0) == first, s)).start()
            pl.when(j < M2_LATE)(lambda: direct(part_of, rec, n, first, sem))

        def go_on(part_of, rec, n, first, sem):
            scopy(j, sem, rec.at[j, :, 0], rec.at[j, :, 0], partner).wait_recv()
            for h in range(2):
                for q, s in ways:
                    sub = pl.ds(q * n, n)
                    mine = part_of(h, s, sub)
                    mine[...] = mine[...] + rec[j, h, 0, sub]
                    scopy(j, sem + 1, mine, rec.at[j, h, 1 + q, sub], to((h == 0) == first, s)).start()
            pl.when(j >= M2_LATE)(lambda: direct(part_of, rec, n, first, sem))

        def s1():
            scopy(j, 0, d2d.at[j], d2d.at[j], partner).wait_recv()
            part[j, c] = part[j, c] + d2d[j]
            begin(big, mrec, nx // 2, True, 1)

        def s2():
            go_on(big, mrec, nx // 2, True, 1)

        def s3():
            rest = mrec.at[j, :, pl.ds(1, 2)]
            scopy(j, 2, rest, rest, partner).wait_recv()
            for h in range(2):
                mine = big(h, 0)
                mine[...] = mine[...] + mrec[j, h, 1] + mrec[j, h, 2]

            @pl.when(j < nch - N_DIRECT)
            def _():
                begin(small, nrec, q_rows, False, 3)

            @pl.when(j >= nch - N_DIRECT)
            def _():
                for h in range(2):
                    for slot, s in enumerate((2, 1, -1)):
                        scopy(j, 4, small(h, s), nrec.at[j, h, slot], to(h == 1, s)).start()

        def s4():
            @pl.when(j < nch - N_DIRECT)
            def _():
                go_on(small, nrec, q_rows, False, 3)

        def s5():
            def finish(slots):
                rest = nrec.at[j, :, pl.ds(3 - slots, slots)]
                scopy(j, 4, rest, rest, partner).wait_recv()
                for h in range(2):
                    val = part[j, c, h, x, y]
                    for slot in range(3 - slots, 3):
                        val = val + nrec[j, h, slot]
                    out[:, pl.ds(pl.multiple_of(j * CW + h * hw, hw), hw)] = val.astype(BF)

            pl.when(j < nch - N_DIRECT)(lambda: finish(2))
            pl.when(j >= nch - N_DIRECT)(lambda: finish(3))

        return s1, s2, s3, s4, s5

    def rs_step(u, carry):
        @pl.when(u < nch)
        def _():
            wd_next(u).wait()
            down_half(u, o)
            scopy(u, 0, part.at[u, o], d2d.at[u], partner).start()

        @pl.when((u >= 2) & (u <= nch))
        def _():
            with jax.named_scope("rs1"):
                stages(u - 1)[0]()

        @pl.when(u < nch)
        def _():
            down_half(u, c)

        @pl.when(u < nch - WD_SLOTS)
        def _():
            wd_next(u + WD_SLOTS).start()

        @pl.when(u == 0)
        def _():
            with jax.named_scope("rs1"):
                stages(0)[0]()

        for n, lag in enumerate(RS_LAGS[1:], 1):
            j = u - lag

            @pl.when((j >= 0) & (j < nch))
            def _():
                with jax.named_scope(f"rs{n + 1}"):
                    stages(j)[n]()
        return carry

    lax.fori_loop(0, nch + max(RS_LAGS), rs_step, 0)
    with jax.named_scope("fin"):
        blocks = nch * (3 + 7 * nx)
        for buf, sem, n in ((xg, ag_send, 1), (part, rs_send, 2)):
            flat = buf.reshape(nch * 2 * n * nx * ny, rows, CW // n).at[pl.ds(0, blocks * n)]
            pltpu.make_async_remote_copy(src_ref=flat, dst_ref=flat, send_sem=sem, recv_sem=sem,
                                         device_id=partner, device_id_type=MESH).wait_send()


def solution(mesh):
    ep_n, ny = mesh.shape["ep"], mesh.shape["tp"]
    nx = ep_n // 2
    row_spec = P(("dp", "ep", "tp"), None)

    def layer(tokens, expert_ids, gates, w_gate, w_up, w_down):
        rows, hid = tokens.shape
        ne, ff, _ = w_down.shape
        group = rows * ep_n * ny
        nch = hid // CW
        dims = (nx, ny, ne, ff, rows, hid)
        vm = pl.BlockSpec(memory_space=pltpu.VMEM)
        hbm = pl.BlockSpec(memory_space=pl.ANY)
        dma = pltpu.SemaphoreType.DMA
        line = ny * rows
        scratch = [
            pltpu.VMEM((rows, hid), BF),
            pltpu.VMEM(expert_ids.shape[::-1], jnp.int32),
            pltpu.VMEM(gates.shape[::-1], F32),
            pltpu.SemaphoreType.DMA((3,)),
            pltpu.VMEM((nch, 2, nx, ny, rows, CW), BF),
            pltpu.VMEM((ep_n, 1, 2 * line), F32),
            pltpu.VMEM((2, nx, ny, 2, 1, 2 * line), F32),
            pltpu.VMEM((group, group), BF),
            pltpu.VMEM((group, CW), BF),
            pltpu.VMEM((nch, ne, 2 * ff, CW), BF),
            pltpu.VMEM((ne // 2, 2 * ff, 2 * (group // ne)), F32),
            pltpu.VMEM((ff, group), BF),
            pltpu.VMEM((group, 128), BF),
            pltpu.VMEM((group, 128), F32),
            pltpu.VMEM((group, ne * ff), BF),
            pltpu.VMEM((WD_SLOTS, ne * ff, CW), BF),
            pltpu.VMEM((nch, 2, 2, nx, ny, rows, CW // 2), F32),
            pltpu.VMEM((nch, 2, nx, ny, rows, CW // 2), F32),
            pltpu.VMEM((nch, 2, 3, nx, rows, CW // 2), F32),
            pltpu.VMEM((nch, 2, 3, rows, CW // 2), F32),
            dma, dma((nch, 5)), dma((3,)), dma((3,)), dma((nch,)), dma((WD_SLOTS,)),
            dma, dma((nch, 5)),
        ]
        return pl.pallas_call(
            functools.partial(kernel, dims),
            out_shape=pltpu.VMEM((rows, hid), BF),
            in_specs=[hbm] * 6,
            out_specs=vm,
            scratch_shapes=scratch,
            compiler_params=pltpu.CompilerParams(collective_id=0, has_side_effects=True,
                                                 vmem_limit_bytes=66_000_000),
        )(tokens, expert_ids.T, gates.T, jnp.swapaxes(w_gate, 1, 2), jnp.swapaxes(w_up, 1, 2),
          w_down.reshape(ne * ff, hid))

    w_spec = P("ep", None, "tp")
    return jax.shard_map(layer, mesh=mesh, in_specs=(row_spec, row_spec, row_spec, w_spec, w_spec, P("ep", "tp", None)),
                         out_specs=row_spec, check_vma=False)
```

```python
import functools

import jax
import jax.numpy as jnp
from jax import lax
from jax.experimental import pallas as pl
from jax.experimental.pallas import tpu as pltpu
from jax.sharding import PartitionSpec as P

MESH = pl.DeviceIdType.MESH
BF = jnp.bfloat16
F32 = jnp.float32
CW = 256
WD_SLOTS = 3
N_DIRECT = 3
DIRECT = 0
FILL = ("m0", "0.0", "0.1", "0.2", "0.3", "0.4", "0.5", "0.6", "0.7", "m1", "1.0", "1.1", "1.2", "1.3", "m2", "2.0",
        "2.1", "1.4", "1.5", "b", "2.2", "2.3", "3.0", "3.1", "1.6", "1.7")
RS_LAGS = (1, 3, 5, 8, 10)
M2_LATE = 8


def kernel(dims, tok_hbm, ids_hbm, gat_hbm, wg, wu, wd, out,
           tok, ids, gat, in_sem, xg, meta_src, meta, pmat, xs, wbuf, acc, h_t, lecol, gcol, hexp, wdbuf,
           part, d2d, mrec, nrec,
           ag_send, ag_recv, meta_send, meta_recv, w_sem, wd_sem, rs_send, rs_recv):
    nx, ny, ne, ff, rows, hid = dims
    nch = hid // CW
    group = 2 * nx * ny * rows
    plane = group // 2
    line = ny * rows
    load = group // ne
    ep_n = 2 * nx
    y = lax.axis_index("tp")
    ep = lax.axis_index("ep")
    x = ep // 2
    c = ep % 2
    o = 1 - c

    def dev(xx, yy, cc):
        return {"tp": yy, "ep": 2 * xx + cc}

    def xo(s):
        return lax.rem(x + s + 2 * nx, nx)

    def yo(s):
        return lax.rem(y + s + 2 * ny, ny)

    def w_copy(k, which):
        src = (wg, wu)[which]
        return pltpu.make_async_copy(src.at[:, :, pl.ds(pl.multiple_of(k * CW, CW) if not isinstance(k, int) else k * CW, CW)],
                                     wbuf.at[k, :, pl.ds(which * ff, ff), :], w_sem.at[k])

    def wd_copy(j):
        return pltpu.make_async_copy(wd.at[:, pl.ds(j * CW, CW)], wdbuf.at[j % WD_SLOTS], wd_sem.at[j % WD_SLOTS])

    barrier = pltpu.get_barrier_semaphore()
    peers = [dev(xo(i), y, c) for i in range(1, nx)] + [dev(x, yo(i), c) for i in range(1, ny)] + [dev(x, y, o)]
    for peer in peers:
        pl.semaphore_signal(barrier, inc=1, device_id=peer, device_id_type=MESH)

    own = [pltpu.make_async_copy(src, dst, in_sem.at[n])
           for n, (src, dst) in enumerate(((ids_hbm, ids), (gat_hbm, gat), (tok_hbm, tok)))]
    for copy in own:
        copy.start()
    with jax.named_scope("w_issue"):
        for k in range(nch):
            for which in range(2):
                w_copy(k, which).start()
        for j in range(WD_SLOTS):
            wd_copy(j).start()

    own[0].wait()
    own[1].wait()
    ids4 = jnp.concatenate([ids[...]] * ny, axis=1)
    gat4 = jnp.concatenate([gat[...]] * ny, axis=1)
    lane = lax.broadcasted_iota(jnp.int32, (1, line), 1)
    mine = (lane // rows) == y
    for p in range(ep_n):
        sel = (ids4 // ne) == p
        le = jnp.sum(jnp.where(sel, ids4 - p * ne, 0).astype(F32), axis=0, keepdims=True)
        ga = jnp.sum(jnp.where(sel, gat4, 0.0), axis=0, keepdims=True)
        meta_src[p, :, pl.ds(0, line)] = jnp.where(mine, le, 0.0)
        meta_src[p, :, pl.ds(line, line)] = jnp.where(mine, ga, 0.0)
    for e2 in range(2):
        meta[c, x, y, e2] = meta_src[2 * x + e2]
    own[2].wait()
    for k in range(nch):
        xg[k, c, x, y] = tok[:, pl.ds(k * CW, CW)]

    acc[...] = jnp.zeros_like(acc)
    with jax.named_scope("barrier"):
        pl.semaphore_wait(barrier, len(peers))

    def mcopy(n, src, dst, to):
        return pltpu.make_async_remote_copy(src_ref=src, dst_ref=dst, send_sem=meta_send.at[n], recv_sem=meta_recv.at[n],
                                            device_id=to, device_id_type=MESH)

    def meta0():
        for i in range(1, nx):
            mcopy(0, meta_src.at[pl.ds(2 * xo(i), 2)], meta.at[c, x, y], dev(xo(i), y, c)).start()

    def meta1():
        whole = meta_src.at[pl.ds(0, 2 * (nx - 1))]
        mcopy(0, whole, whole, dev(x, y, o)).wait()
        for i in range(1, ny):
            mcopy(1, meta.at[c, :, y], meta.at[c, :, y], dev(x, yo(i), c)).start()

    def meta2():
        whole = meta.at[c, :, pl.ds(0, ny - 1)]
        mcopy(1, whole, whole, dev(x, y, o)).wait()
        mcopy(2, meta.at[c], meta.at[c], dev(x, y, o)).start()

    partner = dev(x, y, o)
    hw = CW // 2

    def gather(i, hf, direct=False):
        k = 2 * i + hf

        def first_to(s):
            return dev(xo(s), y, c) if hf == 0 else dev(x, yo(s), c)

        def second_to(s):
            return dev(x, yo(s), c) if hf == 0 else dev(xo(s), y, c)

        def block(s):
            return xg.at[k, c, xo(s), y] if hf == 0 else xg.at[k, c, x, yo(s)]

        def lines(s, cc, sub=slice(None)):
            return xg.at[k, cc, sub, yo(s)] if hf == 0 else xg.at[k, cc, xo(s), sub]

        def rcopy(kind, ref, to, src=None):
            return pltpu.make_async_remote_copy(src_ref=ref if src is None else src, dst_ref=ref, send_sem=ag_send,
                                                recv_sem=ag_recv.at[k, kind], device_id=to, device_id_type=MESH)

        def a0():
            src = tok.at[:, pl.ds(pl.multiple_of(k * CW, CW), CW)]
            for s in (1, -1, 2):
                rcopy(0, block(0), first_to(s), src).start()

        def a1():
            rcopy(0, xg.at[k, c, 0, pl.ds(0, 3)], partner).wait_recv()
            rcopy(1, lines(0, c), second_to(1)).start()
            rcopy(2, lines(0, c), second_to(-1)).start()
            if direct:
                rcopy(3, lines(0, c), second_to(2)).start()
            rcopy(4, lines(0, c), partner).start()

        def a2():
            for n, s in ((1, -1), (2, 1)):
                rcopy(n, lines(s, c), partner).wait_recv()
                if not direct:
                    rcopy(3, lines(s, c, pl.ds((n - 1) * (nx // 2), nx // 2)), second_to(-s)).start()
                rcopy(4, lines(s, c), partner).start()

        def a3():
            rcopy(3, lines(2, c), partner).wait_recv()
            rcopy(4, lines(2, c), partner).start()

        def a4():
            rcopy(4, xg.at[k, o], partner).wait_recv()

        return a0, a1, a2, a3, a4

    n_grp = 2 * nx

    def build_perm():
        mcopy(2, meta.at[c], meta.at[o], dev(x, y, o)).wait()
        les, gas = [], []
        for g in range(n_grp):
            row = meta[g // nx, g % nx, 0, c]
            for i in range(1, ny):
                row = row + meta[g // nx, g % nx, i, c]
            les.append(row[:, :line])
            gas.append(row[:, line:])
        e_iota = lax.broadcasted_iota(jnp.int32, (ne, line), 0).astype(F32)
        hots = [jnp.where(e_iota == le, 1.0, 0.0) for le in les]
        r_i = lax.broadcasted_iota(jnp.int32, (line, line), 0)
        c_i = lax.broadcasted_iota(jnp.int32, (line, line), 1)
        upper = jnp.where(r_i < c_i, 1.0, 0.0).astype(BF)
        before = jnp.dot(jnp.concatenate(hots, axis=0).astype(BF), upper, preferred_element_type=F32)
        off = jnp.zeros((ne, 1), F32)
        s_iota = lax.broadcasted_iota(jnp.int32, (group, line), 0).astype(F32)
        for g in range(n_grp):
            pos = jnp.sum(hots[g] * (e_iota * load + off + before[g * ne:(g + 1) * ne]), axis=0, keepdims=True)
            off = off + jnp.sum(hots[g], axis=1, keepdims=True)
            pmat[:, pl.ds(g * line, line)] = jnp.where(s_iota == pos, 1.0, 0.0).astype(BF)
        le_t = jnp.concatenate(les, axis=0).T
        ga_t = jnp.concatenate(gas, axis=0).T
        for g in range(n_grp):
            lecol[pl.ds(g * line, line), :] = jnp.broadcast_to(le_t[:, g:g + 1], (line, 128)).astype(BF)
            gcol[pl.ds(g * line, line), :] = jnp.broadcast_to(ga_t[:, g:g + 1], (line, 128))

    half_lane = lax.broadcasted_iota(jnp.int32, (2 * ff, 2 * load), 1) < load

    def compute(k):
        pltpu.make_async_copy(wbuf.at[k], wbuf.at[k], w_sem.at[k]).wait()
        xk = xg.at[k].reshape(group, CW)
        with jax.named_scope("perm"):
            for m in range(4):
                sl = pl.ds(m * (group // 4), group // 4)
                xs[sl, :] = jnp.dot(pmat[sl, :], xk[...], preferred_element_type=F32).astype(BF)
        dn = (((1,), (1,)), ((), ()))
        with jax.named_scope("pairs"):
            for p in range(ne // 2):
                rhs = xs[pl.ds(p * 2 * load, 2 * load), :]
                both = wbuf[k, pl.ds(2 * p, 2)].reshape(4 * ff, CW)
                r = lax.dot_general(both, rhs, dn, preferred_element_type=F32)
                acc[p] = acc[p] + jnp.where(half_lane, r[:2 * ff], r[2 * ff:])

    half = nch // 2

    done = [0] * 5
    for event in FILL:
        with jax.named_scope(event):
            if event in ("m0", "m1", "m2", "b"):
                {"m0": meta0, "m1": meta1, "m2": meta2, "b": build_perm}[event]()
            else:
                n, k = (int(v) for v in event.split("."))
                gather(k // 2, k % 2, k < DIRECT)[n]()
                done[n] = k + 1
    assert done[0] == nch

    def steady(i, carry):
        for hf in range(2):
            with jax.named_scope("ag4"):
                gather(i, hf)[4]()
            with jax.named_scope("compute"):
                compute(2 * i + hf)
            for n in range(1, 4):
                hf2 = (hf + done[n]) % 2
                ii = i + (hf + done[n] - hf2) // 2

                @pl.when(ii < half)
                def _():
                    with jax.named_scope(f"ag{n}"):
                        gather(ii, hf2)[n]()
        return carry

    lax.fori_loop(0, half, steady, 0)

    with jax.named_scope("silu"):
        for p in range(ne // 2):
            a = acc[p, :ff, :]
            b = acc[p, ff:, :]
            h_t[:, pl.ds(p * 2 * load, 2 * load)] = (jax.nn.silu(a) * b).astype(BF)
    wide = 4 * ff

    def expand(cc):
        col_e = (lax.broadcasted_iota(jnp.int32, (line, wide), 1) // ff).astype(BF)
        ht = jnp.dot(h_t[...], pmat[:, pl.ds(pl.multiple_of(cc * plane, plane), plane)], preferred_element_type=F32)
        for g in range(plane // line):
            sl = pl.ds(pl.multiple_of(cc * plane + g * line, line), line)
            h = ht[:, g * line:(g + 1) * line].T.astype(BF)
            rep = jnp.concatenate([h] * 4, axis=1)
            le = jnp.concatenate([lecol[sl, :]] * (wide // 128), axis=1)
            for q in range(ne // 4):
                hexp[sl, pl.ds(q * wide, wide)] = jnp.where(col_e + BF(4 * q) == le, rep, BF(0))

    def scopy(j, kind, src, dst, to):
        return pltpu.make_async_remote_copy(src_ref=src, dst_ref=dst, send_sem=rs_send,
                                            recv_sem=rs_recv.at[j, kind], device_id=to, device_id_type=MESH)

    def down_half(j, cc):
        base = pl.multiple_of(cc * plane, plane)

        @pl.when(j == 0)
        def _():
            with jax.named_scope("expand"):
                expand(cc)

        with jax.named_scope("half"):
            n = plane // 2
            for m in range(2):
                sl = pl.ds(pl.multiple_of(base + m * n, n), n)
                v = jnp.dot(hexp[sl, :], wdbuf[lax.rem(j, WD_SLOTS)], preferred_element_type=F32)
                for h in range(2):
                    part[j, cc, h, pl.ds(m * (nx // 2), nx // 2)] = (
                        v[:, h * hw:(h + 1) * hw] * gcol[sl, :]).reshape(nx // 2, ny, rows, hw)

    def wd_next(j):
        slot = lax.rem(j, WD_SLOTS)
        return pltpu.make_async_copy(wd.at[:, pl.ds(pl.multiple_of(j * CW, CW), CW)], wdbuf.at[slot], wd_sem.at[slot])

    def stages(j):
        ways = ((0, 1), (1, -1))
        q_rows = rows // 2

        def big(h, s, sub=slice(None)):
            return part.at[j, c, h, sub, yo(s)] if h == 0 else part.at[j, c, h, xo(s), sub]

        def small(h, s, sub=slice(None)):
            return part.at[j, c, h, xo(s), y, sub] if h == 0 else part.at[j, c, h, x, yo(s), sub]

        def to(along_y, s):
            return dev(x, yo(s), c) if along_y else dev(xo(s), y, c)

        def direct(part_of, rec, n, first, sem):
            for h in range(2):
                for q, s in ways:
                    sub = pl.ds((1 - q) * n, n)
                    scopy(j, sem + 1, part_of(h, s, sub), rec.at[j, h, 1 + q, sub], to((h == 0) == first, s)).start()

        def begin(part_of, rec, n, first, sem):
            for h in range(2):
                for q, s in ways:
                    sub = pl.ds(q * n, n)
                    scopy(j, sem, part_of(h, 2, sub), rec.at[j, h, 0, sub], to((h == 0) == first, s)).start()
            pl.when(j < M2_LATE)(lambda: direct(part_of, rec, n, first, sem))

        def go_on(part_of, rec, n, first, sem):
            scopy(j, sem, rec.at[j, :, 0], rec.at[j, :, 0], partner).wait_recv()
            for h in range(2):
                for q, s in ways:
                    sub = pl.ds(q * n, n)
                    mine = part_of(h, s, sub)
                    mine[...] = mine[...] + rec[j, h, 0, sub]
                    scopy(j, sem + 1, mine, rec.at[j, h, 1 + q, sub], to((h == 0) == first, s)).start()
            pl.when(j >= M2_LATE)(lambda: direct(part_of, rec, n, first, sem))

        def s1():
            scopy(j, 0, d2d.at[j], d2d.at[j], partner).wait_recv()
            part[j, c] = part[j, c] + d2d[j]
            begin(big, mrec, nx // 2, True, 1)

        def s2():
            go_on(big, mrec, nx // 2, True, 1)

        def s3():
            rest = mrec.at[j, :, pl.ds(1, 2)]
            scopy(j, 2, rest, rest, partner).wait_recv()
            for h in range(2):
                mine = big(h, 0)
                mine[...] = mine[...] + mrec[j, h, 1] + mrec[j, h, 2]

            @pl.when(j < nch - N_DIRECT)
            def _():
                begin(small, nrec, q_rows, False, 3)

            @pl.when(j >= nch - N_DIRECT)
            def _():
                for h in range(2):
                    for slot, s in enumerate((2, 1, -1)):
                        scopy(j, 4, small(h, s), nrec.at[j, h, slot], to(h == 1, s)).start()

        def s4():
            @pl.when(j < nch - N_DIRECT)
            def _():
                go_on(small, nrec, q_rows, False, 3)

        def s5():
            def finish(slots):
                rest = nrec.at[j, :, pl.ds(3 - slots, slots)]
                scopy(j, 4, rest, rest, partner).wait_recv()
                for h in range(2):
                    val = part[j, c, h, x, y]
                    for slot in range(3 - slots, 3):
                        val = val + nrec[j, h, slot]
                    out[:, pl.ds(pl.multiple_of(j * CW + h * hw, hw), hw)] = val.astype(BF)

            pl.when(j < nch - N_DIRECT)(lambda: finish(2))
            pl.when(j >= nch - N_DIRECT)(lambda: finish(3))

        return s1, s2, s3, s4, s5

    def rs_step(u, carry):
        @pl.when(u < nch)
        def _():
            wd_next(u).wait()
            down_half(u, o)
            scopy(u, 0, part.at[u, o], d2d.at[u], partner).start()

        @pl.when((u >= 2) & (u <= nch))
        def _():
            with jax.named_scope("rs1"):
                stages(u - 1)[0]()

        @pl.when(u < nch)
        def _():
            down_half(u, c)

        @pl.when(u < nch - WD_SLOTS)
        def _():
            wd_next(u + WD_SLOTS).start()

        @pl.when(u == 0)
        def _():
            with jax.named_scope("rs1"):
                stages(0)[0]()

        for n, lag in enumerate(RS_LAGS[1:], 1):
            j = u - lag

            @pl.when((j >= 0) & (j < nch))
            def _():
                with jax.named_scope(f"rs{n + 1}"):
                    stages(j)[n]()
        return carry

    lax.fori_loop(0, nch + max(RS_LAGS), rs_step, 0)
    with jax.named_scope("fin"):
        blocks = nch * (3 + 7 * nx)
        for buf, sem, n in ((xg, ag_send, 1), (part, rs_send, 2)):
            flat = buf.reshape(nch * 2 * n * nx * ny, rows, CW // n).at[pl.ds(0, blocks * n)]
            pltpu.make_async_remote_copy(src_ref=flat, dst_ref=flat, send_sem=sem, recv_sem=sem,
                                         device_id=partner, device_id_type=MESH).wait_send()


def solution(mesh):
    ep_n, ny = mesh.shape["ep"], mesh.shape["tp"]
    nx = ep_n // 2
    row_spec = P(("dp", "ep", "tp"), None)

    def layer(tokens, expert_ids, gates, w_gate, w_up, w_down):
        rows, hid = tokens.shape
        ne, ff, _ = w_down.shape
        group = rows * ep_n * ny
        nch = hid // CW
        dims = (nx, ny, ne, ff, rows, hid)
        vm = pl.BlockSpec(memory_space=pltpu.VMEM)
        hbm = pl.BlockSpec(memory_space=pl.ANY)
        dma = pltpu.SemaphoreType.DMA
        line = ny * rows
        scratch = [
            pltpu.VMEM((rows, hid), BF),
            pltpu.VMEM(expert_ids.shape[::-1], jnp.int32),
            pltpu.VMEM(gates.shape[::-1], F32),
            pltpu.SemaphoreType.DMA((3,)),
            pltpu.VMEM((nch, 2, nx, ny, rows, CW), BF),
            pltpu.VMEM((ep_n, 1, 2 * line), F32),
            pltpu.VMEM((2, nx, ny, 2, 1, 2 * line), F32),
            pltpu.VMEM((group, group), BF),
            pltpu.VMEM((group, CW), BF),
            pltpu.VMEM((nch, ne, 2 * ff, CW), BF),
            pltpu.VMEM((ne // 2, 2 * ff, 2 * (group // ne)), F32),
            pltpu.VMEM((ff, group), BF),
            pltpu.VMEM((group, 128), BF),
            pltpu.VMEM((group, 128), F32),
            pltpu.VMEM((group, ne * ff), BF),
            pltpu.VMEM((WD_SLOTS, ne * ff, CW), BF),
            pltpu.VMEM((nch, 2, 2, nx, ny, rows, CW // 2), F32),
            pltpu.VMEM((nch, 2, nx, ny, rows, CW // 2), F32),
            pltpu.VMEM((nch, 2, 3, nx, rows, CW // 2), F32),
            pltpu.VMEM((nch, 2, 3, rows, CW // 2), F32),
            dma, dma((nch, 5)), dma((3,)), dma((3,)), dma((nch,)), dma((WD_SLOTS,)),
            dma, dma((nch, 5)),
        ]
        return pl.pallas_call(
            functools.partial(kernel, dims),
            out_shape=pltpu.VMEM((rows, hid), BF),
            in_specs=[hbm] * 6,
            out_specs=vm,
            scratch_shapes=scratch,
            compiler_params=pltpu.CompilerParams(collective_id=0, has_side_effects=True,
                                                 vmem_limit_bytes=66_000_000),
        )(tokens, expert_ids.T, gates.T, jnp.swapaxes(w_gate, 1, 2), jnp.swapaxes(w_up, 1, 2),
          w_down.reshape(ne * ff, hid))

    w_spec = P("ep", None, "tp")
    return jax.shard_map(layer, mesh=mesh, in_specs=(row_spec, row_spec, row_spec, w_spec, w_spec, P("ep", "tp", None)),
                         out_specs=row_spec, check_vma=False)
```
